32 devices in a mesh: ga: 8 (over z, y), ba: 4 (over x, core).
Axes of the slice: x: 2, y: 2, z: 4, core: 2. Of those that a mesh axis runs over, the one named last changes fastest.
Arguments:
- coefficients: bfloat16 [10240, 6144], P('ga', 'ba')
- rotation: bfloat16 [6144, 6144], P('ga', 'ba'), may hold values from -0.078125 to 0.078125
Outputs:
- new_coefficients: bfloat16 [10240, 6144], P('ga', 'ba')
- band_rms: float32 [6144], P('ba')
The draws below stay inside these ranges and needn't reach their ends.
All inputs are finite; a program needn't handle non-finite values.
Results may differ from the reference program's by a relative error of at most 0.0004.
Values may be sent and summed in bfloat16 or wider, within the bound.
A program may use at most 128 MiB of HBM per device.

```python
import math
import jax
import jax.numpy as jnp
from jax import lax

NB = 6144
NG = 10240


def draw_coefficients(key, part):
    first, second, third = jax.random.split(jax.random.fold_in(key, 11), 3)
    positions = jnp.arange(NG, dtype=jnp.float32)[:, None]
    row_scale = jnp.exp(positions / NG * math.log(3.0)) * jnp.exp(jax.random.uniform(first, (NG, 1), jnp.float32) * math.log(3.3))
    col_scale = jnp.exp(jax.random.uniform(second, (1, NB), jnp.float32) * math.log(10.0))
    base = jnp.clip(jax.random.normal(third, (NG, NB), jnp.float32), -6.0, 6.0)
    return (base * row_scale * col_scale).astype(jnp.bfloat16)


def steps_of(own_key, shape, shards, least, largest):
    loudness = 1.0
    for axis_at, parts in shards:
        heights = jax.random.uniform(jax.random.fold_in(jax.random.fold_in(own_key, 6), axis_at), (parts,), jnp.float32, least / len(shards), largest / len(shards))
        loudness = loudness * jnp.repeat(jnp.exp(heights), shape[axis_at] // parts).reshape((-1,) + (1,) * (len(shape) - 1 - axis_at))
    return loudness


def normal_values(own_key, shape, deviation, limit, shards=(), kind=jnp.bfloat16):
    drawn = jax.random.normal(own_key, shape, jnp.float32) * deviation
    if len(shards) > 0:
        drawn = steps_of(own_key, shape, shards, -0.22, 0.18) * drawn
    return jnp.clip(drawn, min=-limit, max=limit).astype(kind)


def setup_inputs(seed: int = 0) -> dict:
    seeds = jax.random.split(jax.random.key(seed), 3)
    coefficients = draw_coefficients(jax.random.fold_in(seeds[2], 71), 0)
    rotation = normal_values(seeds[1], (NB, NB), NB ** -0.5, 0.078125, ((0, 8), (1, 4)))
    return {"coefficients": coefficients, "rotation": rotation}


def reference(coefficients, rotation):
    rotated = jnp.dot(coefficients, rotation, preferred_element_type=jnp.float32)
    sums = lax.optimization_barrier(jnp.sum(rotated * rotated, axis=0))
    band_rms = jnp.sqrt(sums / NG + 1e-06)
    return ((rotated / band_rms).astype(jnp.bfloat16), band_rms)
```

```python
import functools
import math

import jax
import jax.numpy as jnp
from jax import lax
from jax.experimental import pallas as pl
from jax.experimental.pallas import tpu as pltpu
from jax.sharding import PartitionSpec as P

MESH = pl.DeviceIdType.MESH
CHUNKS = 6


def kernel(n_ga, n_ba, line, coef, rot, out, rms_out, a_buf, b_buf, total, stats,
           recv, send_z, send_zb, send_y, a_recv, a_send_x, a_send_p, s_recv, s_send, own):
    lanes = n_ga // line
    depth = rot.shape[0]
    rows, width = coef.shape
    piece = depth // CHUNKS
    span = lanes * depth
    me, mb = lax.axis_index("ga"), lax.axis_index("ba")
    z, w = me // lanes, lax.rem(me, lanes)
    bx, bc = mb // 2, lax.rem(mb, 2)
    half = n_ba // 2

    def ga(i):
        return {"ga": i}

    def side(o):
        return lax.rem(w + o, lanes)

    def chunk(index):
        return b_buf.at[pl.ds(pl.multiple_of(index * piece, piece), piece)]

    barrier = pltpu.get_barrier_semaphore()
    for o in range(1, n_ga):
        pl.semaphore_signal(barrier, inc=1, device_id=ga(lax.rem(me + o, n_ga)), device_id_type=MESH)
    for o in range(1, n_ba):
        pl.semaphore_signal(barrier, inc=1, device_id={"ba": lax.rem(mb + o, n_ba)}, device_id_type=MESH)

    mine = [
        pltpu.make_async_copy(rot, b_buf.at[pl.ds(pl.multiple_of(me * depth, depth), depth)], own.at[0]),
        pltpu.make_async_copy(coef, a_buf.at[mb], own.at[1]),
    ]
    for copy in mine:
        copy.start()
    pl.semaphore_wait(barrier, n_ga - 1 + n_ba - 1)

    def remote(src, index, sem, target):
        return pltpu.make_async_remote_copy(
            src_ref=src, dst_ref=chunk(index), send_sem=sem, recv_sem=recv.at[index],
            device_id=ga(target), device_id_type=MESH)

    def arrived(index):
        pltpu.make_async_copy(chunk(index), chunk(index), recv.at[index]).wait()

    def along(k, src, index, sem):
        @pl.when(z < line - 1 if k == 0 else z > 0)
        def _():
            remote(src, index, sem, me + lanes if k == 0 else me - lanes).start()

    def across(src, index, from_z):
        for o in range(1, lanes):
            remote(src, index, send_y.at[o - 1, from_z], z * lanes + side(o)).start()

    def own_chunk(q):
        return rot.at[pl.ds(q * piece, piece)]

    last = CHUNKS - 1
    across(own_chunk(last), me * CHUNKS + last, z)
    for q in range(CHUNKS):
        for k in range(2):
            along(k, own_chunk(q), me * CHUNKS + q, send_z.at[k, z])
        if q < last:
            across(own_chunk(q), me * CHUNKS + q, z)

    def a_copy(src, index, sem, target):
        return pltpu.make_async_remote_copy(
            src_ref=src, dst_ref=a_buf.at[index], send_sem=sem, recv_sem=a_recv.at[index],
            device_id={"ba": target}, device_id_type=MESH)

    partner = mb + 1 - 2 * bc
    far = [lax.rem(bx + o, half) * 2 + bc for o in range(1, half)]
    for o, target in enumerate(far):
        a_copy(coef, mb, a_send_x.at[o], target).start()
    a_copy(coef, mb, a_send_p.at[mb], partner).start()

    for o in range(1, lanes):
        index = (z * lanes + side(o)) * CHUNKS + last
        arrived(index)
        for k in range(2):
            along(k, chunk(index), index, send_zb.at[k, z * lanes + side(o)])

    tile = math.gcd(rows, 256)

    def multiply(j, dist):
        from_z = z - dist + 2 * dist * j

        @pl.when((from_z >= 0) & (from_z < line) & ((dist > 0) | (j == 0)))
        def _():
            for o in range(1, lanes):
                for q in range(last):
                    arrived((from_z * lanes + side(o)) * CHUNKS + q)
            begin = from_z * span
            at, column = begin // width, pl.multiple_of(lax.rem(begin, width), 128)

            @pl.loop(0, rows // tile)
            def _(t):
                part = pl.ds(pl.multiple_of(t * tile, tile), tile)
                product = jnp.dot(
                    a_buf[at, part, pl.ds(column, span)],
                    b_buf[pl.ds(pl.multiple_of(begin, span), span), :],
                    preferred_element_type=jnp.float32)

                @pl.when(dist == 0)
                def _():
                    total[part, :] = product

                @pl.when(dist > 0)
                def _():
                    total[part, :] += product

    def at_distance(dist):
        lax.fori_loop(0, 2, lambda j, c: (multiply(j, dist), c)[1], 0)

    def relay(d, carry):
        for q in range(CHUNKS + lanes - 1):
            for k in range(2):
                from_z = z - d if k == 0 else z + d

                @pl.when((from_z >= 0) & (from_z < line))
                def _():
                    lane = w if q < CHUNKS else side(q - CHUNKS + 1)
                    block = from_z * lanes + lane
                    index = block * CHUNKS + min(q, last)
                    arrived(index)
                    along(k, chunk(index), index, send_z.at[k, from_z] if q < CHUNKS else send_zb.at[k, block])
                    if q < last:
                        across(chunk(index), index, from_z)

            if q == 2:
                @pl.when(d == 2)
                def _():
                    for source in far:
                        pltpu.make_async_copy(a_buf.at[source], a_buf.at[source], a_recv.at[source]).wait()
                        a_copy(a_buf.at[source], source, a_send_p.at[source], partner).start()

            if q == 1:
                @pl.when(d == line - 1)
                def _():
                    at_distance(line - 3)

            if q == last:
                @pl.when(d == 2)
                def _():
                    for copy in mine:
                        copy.wait()
                    for x in range(half):
                        source = x * 2 + 1 - bc
                        pltpu.make_async_copy(a_buf.at[source], a_buf.at[source], a_recv.at[source]).wait()

                @pl.when(d >= 2)
                def _():
                    at_distance(d - 2 + d // (line - 1))
        return carry

    lax.fori_loop(1, line, relay, 0)
    at_distance(line - 1)

    def squares(t, c):
        v = total[pl.ds(pl.multiple_of(t * tile, tile), tile), :]
        return c + jnp.sum(v * v, axis=0, keepdims=True)

    stats[me] = lax.fori_loop(0, rows // tile, squares, jnp.zeros((1, total.shape[1]), jnp.float32))

    def share(o, target, slot):
        return pltpu.make_async_remote_copy(
            src_ref=stats.at[me], dst_ref=stats.at[me], send_sem=s_send.at[o], recv_sem=s_recv.at[slot],
            device_id=ga(target), device_id_type=MESH)

    for o in range(1, n_ga):
        share(o, lax.rem(me + o, n_ga), me).start()
    for o in range(1, n_ga):
        source = lax.rem(me + o, n_ga)
        pltpu.make_async_copy(stats.at[source], stats.at[source], s_recv.at[source]).wait()
    everything = stats[0]
    for g in range(1, n_ga):
        everything = everything + stats[g]
    rms = jnp.sqrt(everything / (rows * n_ga) + 1e-06)
    rms_out[...] = rms
    scale = 1.0 / rms

    @pl.loop(0, rows // tile)
    def _(t):
        part = pl.ds(pl.multiple_of(t * tile, tile), tile)
        out[part, :] = (total[part, :] * scale).astype(jnp.bfloat16)

    for o in range(1, n_ga):
        share(o, lax.rem(me + o, n_ga), me).wait_send()
    for o, target in enumerate(far):
        a_copy(coef, mb, a_send_x.at[o], target).wait_send()
    for x in range(half):
        a_copy(coef, x * 2 + bc, a_send_p.at[x * 2 + bc], partner).wait_send()

    def sent(count, sem):
        view = b_buf.at[pl.ds(0, count * piece)]
        pltpu.make_async_copy(view, view, sem).wait()

    for from_z in range(line):
        for k in range(2):
            @pl.when((z >= from_z) & (z < line - 1) if k == 0 else (z <= from_z) & (z > 0))
            def _():
                sent(CHUNKS, send_z.at[k, from_z])
                for o in range(1, lanes):
                    sent(1, send_zb.at[k, from_z * lanes + side(o)])
        for o in range(1, lanes):
            @pl.when(z == from_z)
            def _():
                sent(CHUNKS, send_y.at[o - 1, from_z])

            @pl.when(z != from_z)
            def _():
                sent(last, send_y.at[o - 1, from_z])


def solution(mesh):
    n_ga, n_ba = mesh.shape["ga"], mesh.shape["ba"]
    line = 2 ** math.ceil(math.log2(n_ga) / 2)
    lanes = n_ga // line

    def body(coef, rot):
        rows, width = coef.shape
        depth, columns = rot.shape
        dma = pltpu.SemaphoreType.DMA
        out, rms = pl.pallas_call(
            functools.partial(kernel, n_ga, n_ba, line),
            out_shape=(jax.ShapeDtypeStruct((rows, columns), jnp.bfloat16),
                       jax.ShapeDtypeStruct((1, columns), jnp.float32)),
            in_specs=[pl.BlockSpec(memory_space=pl.ANY)] * 2,
            out_specs=(pl.BlockSpec(memory_space=pltpu.VMEM),) * 2,
            scratch_shapes=[
                pltpu.VMEM((n_ba, rows, width), jnp.bfloat16),
                pltpu.VMEM((n_ga * depth, columns), jnp.bfloat16),
                pltpu.VMEM((rows, columns), jnp.float32),
                pltpu.VMEM((n_ga, 1, columns), jnp.float32),
                dma((n_ga * CHUNKS,)),
                dma((2, line)),
                dma((2, n_ga)),
                dma((lanes - 1, line)),
                dma((n_ba,)),
                dma((n_ba // 2 - 1,)),
                dma((n_ba,)),
                dma((n_ga,)),
                dma((n_ga,)),
                dma((2,)),
            ],
            compiler_params=pltpu.CompilerParams(
                collective_id=0, has_side_effects=True, vmem_limit_bytes=67043328),
        )(coef, rot)
        return out, rms.reshape(columns)

    return jax.shard_map(body, mesh=mesh, in_specs=(P("ga", "ba"), P("ga", "ba")),
                         out_specs=(P("ga", "ba"), P("ba")), check_vma=False)
```

```python
import functools
import math

import jax
import jax.numpy as jnp
from jax import lax
from jax.experimental import pallas as pl
from jax.experimental.pallas import tpu as pltpu
from jax.sharding import PartitionSpec as P

MESH = pl.DeviceIdType.MESH
CHUNKS = 6
CROSS = 1


def kernel(n_ga, n_ba, line, coef, rot, total, rms_out, a_buf, b_buf, stats,
           recv, send_z, send_zb, send_y, a_recv, a_send_x, a_send_p, s_recv, s_send, own):
    lanes = n_ga // line
    depth = rot.shape[0]
    rows, width = coef.shape
    piece = depth // CHUNKS
    span = lanes * depth
    me, mb = lax.axis_index("ga"), lax.axis_index("ba")
    z, w = me // lanes, lax.rem(me, lanes)
    bx, bc = mb // 2, lax.rem(mb, 2)
    half = n_ba // 2

    def ga(i):
        return {"ga": i}

    def side(o):
        return lax.rem(w + o, lanes)

    def chunk(index):
        return b_buf.at[pl.ds(pl.multiple_of(index * piece, piece), piece)]

    barrier = pltpu.get_barrier_semaphore()
    for o in range(1, n_ga):
        pl.semaphore_signal(barrier, inc=1, device_id=ga(lax.rem(me + o, n_ga)), device_id_type=MESH)
    for o in range(1, n_ba):
        pl.semaphore_signal(barrier, inc=1, device_id={"ba": lax.rem(mb + o, n_ba)}, device_id_type=MESH)

    mine = [
        pltpu.make_async_copy(rot, b_buf.at[pl.ds(pl.multiple_of(me * depth, depth), depth)], own.at[0]),
        pltpu.make_async_copy(coef, a_buf.at[mb], own.at[1]),
    ]
    for copy in mine:
        copy.start()
    pl.semaphore_wait(barrier, n_ga - 1 + n_ba - 1)

    def remote(src, index, sem, target):
        return pltpu.make_async_remote_copy(
            src_ref=src, dst_ref=chunk(index), send_sem=sem, recv_sem=recv.at[index],
            device_id=ga(target), device_id_type=MESH)

    def arrived(index):
        pltpu.make_async_copy(chunk(index), chunk(index), recv.at[index]).wait()

    def along(k, src, index, sem):
        @pl.when(z < line - 1 if k == 0 else z > 0)
        def _():
            remote(src, index, sem, me + lanes if k == 0 else me - lanes).start()

    def across(src, index, from_z):
        for o in range(1, lanes):
            remote(src, index, send_y.at[o - 1, from_z], z * lanes + side(o)).start()

    def own_chunk(q):
        return rot.at[pl.ds(q * piece, piece)]

    last = CHUNKS - CROSS
    crossed = [(o, q) for q in range(last, CHUNKS) for o in range(1, lanes)]
    for q in range(last, CHUNKS):
        across(own_chunk(q), me * CHUNKS + q, z)
    for q in range(CHUNKS):
        for k in range(2):
            along(k, own_chunk(q), me * CHUNKS + q, send_z.at[k, z])
        if q < last:
            across(own_chunk(q), me * CHUNKS + q, z)

    def a_copy(src, index, sem, target):
        return pltpu.make_async_remote_copy(
            src_ref=src, dst_ref=a_buf.at[index], send_sem=sem, recv_sem=a_recv.at[index],
            device_id={"ba": target}, device_id_type=MESH)

    partner = mb + 1 - 2 * bc
    far = [lax.rem(bx + o, half) * 2 + bc for o in range(1, half)]
    for o, target in enumerate(far):
        a_copy(coef, mb, a_send_x.at[o], target).start()
    a_copy(coef, mb, a_send_p.at[mb], partner).start()

    for o, q in crossed:
        index = (z * lanes + side(o)) * CHUNKS + q
        arrived(index)
        for k in range(2):
            along(k, chunk(index), index, send_zb.at[k, z * lanes + side(o)])

    tile = math.gcd(rows, 256)

    def multiply(j, dist, part):
        from_z = z - dist + 2 * dist * j

        @pl.when((from_z >= 0) & (from_z < line) & ((dist > 0) | (j == 0)))
        def _():
            if part == "all":
                for o in range(1, lanes):
                    for q in range(last):
                        arrived((from_z * lanes + side(o)) * CHUNKS + q)
                panel(from_z * span, span, dist)
                return
            if part == "own":
                panel((from_z * lanes + w) * depth, depth, dist)
                return
            for o in range(1, lanes):
                block = from_z * lanes + side(o)
                for q in range(cut):
                    arrived(block * CHUNKS + q)
                panel(block * depth, cut * piece, dist)
                for q in range(cut, last):
                    arrived(block * CHUNKS + q)
                panel(block * depth + cut * piece, depth - cut * piece, dist)

    cut = max(q for q in range(last) if q * piece % 128 == 0) if depth % 128 == 0 else 0

    def panel(begin, size, dist):
        at, column = begin // width, pl.multiple_of(lax.rem(begin, width), 128)

        @pl.loop(0, rows // tile)
        def _(t):
            part = pl.ds(pl.multiple_of(t * tile, tile), tile)
            product = jnp.dot(
                a_buf[at, part, pl.ds(column, size)],
                b_buf[pl.ds(pl.multiple_of(begin, 128), size), :],
                preferred_element_type=jnp.float32)

            @pl.when(dist == 0)
            def _():
                total[part, :] = product

            @pl.when(dist > 0)
            def _():
                total[part, :] += product

    def at_distance(dist, part="all"):
        if cut == 0:
            if part == "own":
                return
            part = "all"
        lax.fori_loop(0, 2, lambda j, c: (multiply(j, dist, part), c)[1], 0)

    def relay(d, carry):
        for step, (o, q) in enumerate([(0, q) for q in range(CHUNKS)] + crossed):
            for k in range(2):
                from_z = z - d if k == 0 else z + d

                @pl.when((from_z >= 0) & (from_z < line))
                def _():
                    block = from_z * lanes + side(o)
                    index = block * CHUNKS + q
                    arrived(index)
                    along(k, chunk(index), index, send_zb.at[k, block] if o else send_z.at[k, from_z])
                    if q < last:
                        across(chunk(index), index, from_z)

            if step == CHUNKS // 3:
                @pl.when(d == 2)
                def _():
                    for source in far:
                        pltpu.make_async_copy(a_buf.at[source], a_buf.at[source], a_recv.at[source]).wait()
                        a_copy(a_buf.at[source], source, a_send_p.at[source], partner).start()

            if step == CHUNKS // 6:
                @pl.when(d == line - 1)
                def _():
                    at_distance(line - 3)

            for when, dist, part in ((CHUNKS // 2, line - 2, "own"), (CHUNKS - 2, line - 2, "others"),
                                     (CHUNKS - 1, line - 1, "own")):
                if step == when:
                    @pl.when(d == line - 1)
                    def _():
                        at_distance(dist, part)

            if step == CHUNKS - 1:
                @pl.when(d == 2)
                def _():
                    for copy in mine:
                        copy.wait()
                    for x in range(half):
                        source = x * 2 + 1 - bc
                        pltpu.make_async_copy(a_buf.at[source], a_buf.at[source], a_recv.at[source]).wait()

                @pl.when((d >= 2) & (d < line - 1))
                def _():
                    at_distance(d - 2)
        return carry

    lax.fori_loop(1, line, relay, 0)
    at_distance(line - 1, "others")

    def squares(t, c):
        v = total[pl.ds(pl.multiple_of(t * tile, tile), tile), :]
        return c + jnp.sum(v * v, axis=0, keepdims=True)

    stats[me] = lax.fori_loop(0, rows // tile, squares, jnp.zeros((1, total.shape[1]), jnp.float32))

    def share(o, target, slot):
        return pltpu.make_async_remote_copy(
            src_ref=stats.at[me], dst_ref=stats.at[me], send_sem=s_send.at[o], recv_sem=s_recv.at[slot],
            device_id=ga(target), device_id_type=MESH)

    for o in range(1, n_ga):
        share(o, lax.rem(me + o, n_ga), me).start()
    for o in range(1, n_ga):
        source = lax.rem(me + o, n_ga)
        pltpu.make_async_copy(stats.at[source], stats.at[source], s_recv.at[source]).wait()
    everything = stats[0]
    for g in range(1, n_ga):
        everything = everything + stats[g]
    rms = jnp.sqrt(everything / (rows * n_ga) + 1e-06)
    rms_out[...] = rms
    for o in range(1, n_ga):
        share(o, lax.rem(me + o, n_ga), me).wait_send()
    for o, target in enumerate(far):
        a_copy(coef, mb, a_send_x.at[o], target).wait_send()
    for x in range(half):
        a_copy(coef, x * 2 + bc, a_send_p.at[x * 2 + bc], partner).wait_send()

    def sent(count, sem):
        view = b_buf.at[pl.ds(0, count * piece)]
        pltpu.make_async_copy(view, view, sem).wait()

    for from_z in range(line):
        for k in range(2):
            @pl.when((z >= from_z) & (z < line - 1) if k == 0 else (z <= from_z) & (z > 0))
            def _():
                sent(CHUNKS, send_z.at[k, from_z])
                for o in range(1, lanes):
                    sent(CROSS, send_zb.at[k, from_z * lanes + side(o)])
        for o in range(1, lanes):
            @pl.when(z == from_z)
            def _():
                sent(CHUNKS, send_y.at[o - 1, from_z])

            @pl.when(z != from_z)
            def _():
                sent(last, send_y.at[o - 1, from_z])


def solution(mesh):
    n_ga, n_ba = mesh.shape["ga"], mesh.shape["ba"]
    line = 2 ** math.ceil(math.log2(n_ga) / 2)
    lanes = n_ga // line

    def body(coef, rot):
        rows, width = coef.shape
        depth, columns = rot.shape
        dma = pltpu.SemaphoreType.DMA
        rotated, rms = pl.pallas_call(
            functools.partial(kernel, n_ga, n_ba, line),
            out_shape=(pltpu.VMEM((rows, columns), jnp.float32),
                       pltpu.VMEM((1, columns), jnp.float32)),
            in_specs=[pl.BlockSpec(memory_space=pltpu.HBM)] * 2,
            out_specs=(pl.BlockSpec(memory_space=pltpu.VMEM),) * 2,
            scratch_shapes=[
                pltpu.VMEM((n_ba, rows, width), jnp.bfloat16),
                pltpu.VMEM((n_ga * depth, columns), jnp.bfloat16),
                pltpu.VMEM((n_ga, 1, columns), jnp.float32),
                dma((n_ga * CHUNKS,)),
                dma((2, line)),
                dma((2, n_ga)),
                dma((lanes - 1, line)),
                dma((n_ba,)),
                dma((n_ba // 2 - 1,)),
                dma((n_ba,)),
                dma((n_ga,)),
                dma((n_ga,)),
                dma((2,)),
            ],
            compiler_params=pltpu.CompilerParams(
                collective_id=0, has_side_effects=True, vmem_limit_bytes=48 * 2**20),
        )(*(pltpu.with_memory_space_constraint(x, pltpu.HBM) for x in (coef, rot)))
        return (rotated * (1.0 / rms)).astype(jnp.bfloat16), rms.reshape(columns)

    return jax.shard_map(body, mesh=mesh, in_specs=(P("ga", "ba"), P("ga", "ba")),
                         out_specs=(P("ga", "ba"), P("ba")), check_vma=False)
```

```python
import functools
import math

import jax
import jax.numpy as jnp
from jax import lax
from jax.experimental import pallas as pl
from jax.experimental.pallas import tpu as pltpu
from jax.sharding import PartitionSpec as P

MESH = pl.DeviceIdType.MESH
CHUNKS = 6
CROSS = 1


def kernel(n_ga, n_ba, line, coef, rot, total, rms_out, a_buf, b_buf, stats,
           recv, send_z, send_zb, send_y, a_recv, a_send_x, a_send_p, s_recv, s_send, own):
    lanes = n_ga // line
    depth = rot.shape[0]
    rows, width = coef.shape
    piece = depth // CHUNKS
    span = lanes * depth
    me, mb = lax.axis_index("ga"), lax.axis_index("ba")
    z, w = me // lanes, lax.rem(me, lanes)
    bx, bc = mb // 2, lax.rem(mb, 2)
    half = n_ba // 2

    def ga(i):
        return {"ga": i}

    def side(o):
        return lax.rem(w + o, lanes)

    def chunk(index):
        return b_buf.at[pl.ds(pl.multiple_of(index * piece, piece), piece)]

    partner = mb + 1 - 2 * bc
    far = [lax.rem(bx + o, half) * 2 + bc for o in range(1, half)]

    barrier = pltpu.get_barrier_semaphore()
    def greet(device):
        pl.semaphore_signal(barrier, inc=1, device_id=device, device_id_type=MESH)

    @pl.when(z > 0)
    def _():
        greet(ga(me - lanes))

    @pl.when(z < line - 1)
    def _():
        greet(ga(me + lanes))

    for o in range(1, lanes):
        greet(ga(z * lanes + side(o)))
    for target in [*far, partner]:
        greet({"ba": target})

    mine = [
        pltpu.make_async_copy(rot, b_buf.at[pl.ds(pl.multiple_of(me * depth, depth), depth)], own.at[0]),
        pltpu.make_async_copy(coef, a_buf.at[mb], own.at[1]),
    ]
    for copy in mine:
        copy.start()
    ends = (line - 1 - z) // (line - 1) + z // (line - 1)
    pl.semaphore_wait(barrier, 2 - ends + lanes - 1 + len(far) + 1)

    def remote(src, index, sem, target):
        return pltpu.make_async_remote_copy(
            src_ref=src, dst_ref=chunk(index), send_sem=sem, recv_sem=recv.at[index],
            device_id=ga(target), device_id_type=MESH)

    def arrived(index):
        pltpu.make_async_copy(chunk(index), chunk(index), recv.at[index]).wait()

    def along(k, src, index, sem):
        @pl.when(z < line - 1 if k == 0 else z > 0)
        def _():
            remote(src, index, sem, me + lanes if k == 0 else me - lanes).start()

    def across(src, index, from_z):
        for o in range(1, lanes):
            remote(src, index, send_y.at[o - 1, from_z], z * lanes + side(o)).start()

    def own_chunk(q):
        return rot.at[pl.ds(q * piece, piece)]

    last = CHUNKS - CROSS
    crossed = [(o, q) for q in range(last, CHUNKS) for o in range(1, lanes)]
    for q in range(last, CHUNKS):
        across(own_chunk(q), me * CHUNKS + q, z)
    for q in range(CHUNKS):
        for k in range(2):
            along(k, own_chunk(q), me * CHUNKS + q, send_z.at[k, z])
        if q < last:
            across(own_chunk(q), me * CHUNKS + q, z)

    def a_copy(src, index, sem, target):
        return pltpu.make_async_remote_copy(
            src_ref=src, dst_ref=a_buf.at[index], send_sem=sem, recv_sem=a_recv.at[index],
            device_id={"ba": target}, device_id_type=MESH)

    for o, target in enumerate(far):
        a_copy(coef, mb, a_send_x.at[o], target).start()
    a_copy(coef, mb, a_send_p.at[mb], partner).start()

    for o, q in crossed:
        index = (z * lanes + side(o)) * CHUNKS + q
        arrived(index)
        for k in range(2):
            along(k, chunk(index), index, send_zb.at[k, z * lanes + side(o)])

    tile = math.gcd(rows, 256)

    def multiply(j, dist, part):
        from_z = z - dist + 2 * dist * j

        @pl.when((from_z >= 0) & (from_z < line) & ((dist > 0) | (j == 0)))
        def _():
            if part == "all":
                for o in range(1, lanes):
                    for q in range(last):
                        arrived((from_z * lanes + side(o)) * CHUNKS + q)
                panel(from_z * span, span, dist)
                return
            if part == "own":
                panel((from_z * lanes + w) * depth, depth, dist)
                return
            for o in range(1, lanes):
                block = from_z * lanes + side(o)
                for q in range(cut) if part == "cut" else range(cut, last):
                    arrived(block * CHUNKS + q)
                if part == "cut":
                    panel(block * depth, cut * piece, dist)
                else:
                    panel(block * depth + cut * piece, depth - cut * piece, dist)

    cut = max(q for q in range(last) if q * piece % 128 == 0) if depth % 128 == 0 else 0

    def panel(begin, size, dist):
        at, column = begin // width, pl.multiple_of(lax.rem(begin, width), 128)

        @pl.loop(0, rows // tile)
        def _(t):
            part = pl.ds(pl.multiple_of(t * tile, tile), tile)
            product = jnp.dot(
                a_buf[at, part, pl.ds(column, size)],
                b_buf[pl.ds(pl.multiple_of(begin, 128), size), :],
                preferred_element_type=jnp.float32)

            @pl.when(dist == 0)
            def _():
                total[part, :] = product

            @pl.when(dist > 0)
            def _():
                total[part, :] += product

    def at_distance(dist, part="all"):
        if cut == 0:
            if part in ("own", "cut"):
                return
            part = "all"
        lax.fori_loop(0, 2, lambda j, c: (multiply(j, dist, part), c)[1], 0)

    def relay(d, carry):
        for step, (o, q) in enumerate([(0, q) for q in range(CHUNKS)] + crossed):
            for k in range(2):
                from_z = z - d if k == 0 else z + d

                @pl.when((from_z >= 0) & (from_z < line))
                def _():
                    block = from_z * lanes + side(o)
                    index = block * CHUNKS + q
                    arrived(index)
                    along(k, chunk(index), index, send_zb.at[k, block] if o else send_z.at[k, from_z])
                    if q < last:
                        across(chunk(index), index, from_z)

            if step == CHUNKS // 3:
                @pl.when(d == 2)
                def _():
                    for source in far:
                        pltpu.make_async_copy(a_buf.at[source], a_buf.at[source], a_recv.at[source]).wait()
                        a_copy(a_buf.at[source], source, a_send_p.at[source], partner).start()

            if step == CHUNKS // 6:
                @pl.when(d == line - 1)
                def _():
                    at_distance(line - 3)

            for when, dist, part in ((CHUNKS // 2, line - 2, "own"), (CHUNKS - 2, line - 2, "cut"),
                                     (CHUNKS - 2, line - 2, "rest"), (CHUNKS - 1, line - 1, "own"),
                                     (CHUNKS - 1, line - 1, "cut")):
                if step == when:
                    @pl.when(d == line - 1)
                    def _():
                        at_distance(dist, part)

            if step == CHUNKS - 1:
                @pl.when(d == 2)
                def _():
                    for copy in mine:
                        copy.wait()
                    for x in range(half):
                        source = x * 2 + 1 - bc
                        pltpu.make_async_copy(a_buf.at[source], a_buf.at[source], a_recv.at[source]).wait()

                @pl.when((d >= 2) & (d < line - 1))
                def _():
                    at_distance(d - 2)
        return carry

    lax.fori_loop(1, line, relay, 0)
    at_distance(line - 1, "rest")

    def squares(t, c):
        v = total[pl.ds(pl.multiple_of(t * tile, tile), tile), :]
        return c + jnp.sum(v * v, axis=0, keepdims=True)

    stats[me] = lax.fori_loop(0, rows // tile, squares, jnp.zeros((1, total.shape[1]), jnp.float32))

    def share(o, target, slot):
        return pltpu.make_async_remote_copy(
            src_ref=stats.at[me], dst_ref=stats.at[me], send_sem=s_send.at[o], recv_sem=s_recv.at[slot],
            device_id=ga(target), device_id_type=MESH)

    for o in range(1, n_ga):
        share(o, lax.rem(me + o, n_ga), me).start()
    for o in range(1, n_ga):
        source = lax.rem(me + o, n_ga)
        pltpu.make_async_copy(stats.at[source], stats.at[source], s_recv.at[source]).wait()
    everything = stats[0]
    for g in range(1, n_ga):
        everything = everything + stats[g]
    rms = jnp.sqrt(everything / (rows * n_ga) + 1e-06)
    rms_out[...] = rms
    for o in range(1, n_ga):
        share(o, lax.rem(me + o, n_ga), me).wait_send()
    for o, target in enumerate(far):
        a_copy(coef, mb, a_send_x.at[o], target).wait_send()
    for x in range(half):
        a_copy(coef, x * 2 + bc, a_send_p.at[x * 2 + bc], partner).wait_send()

    def sent(count, sem):
        view = b_buf.at[pl.ds(0, count * piece)]
        pltpu.make_async_copy(view, view, sem).wait()

    for from_z in range(line):
        for k in range(2):
            @pl.when((z >= from_z) & (z < line - 1) if k == 0 else (z <= from_z) & (z > 0))
            def _():
                sent(CHUNKS, send_z.at[k, from_z])
                for o in range(1, lanes):
                    sent(CROSS, send_zb.at[k, from_z * lanes + side(o)])
        for o in range(1, lanes):
            @pl.when(z == from_z)
            def _():
                sent(CHUNKS, send_y.at[o - 1, from_z])

            @pl.when(z != from_z)
            def _():
                sent(last, send_y.at[o - 1, from_z])


def solution(mesh):
    n_ga, n_ba = mesh.shape["ga"], mesh.shape["ba"]
    line = 2 ** math.ceil(math.log2(n_ga) / 2)
    lanes = n_ga // line

    def body(coef, rot):
        rows, width = coef.shape
        depth, columns = rot.shape
        dma = pltpu.SemaphoreType.DMA
        rotated, rms = pl.pallas_call(
            functools.partial(kernel, n_ga, n_ba, line),
            out_shape=(pltpu.VMEM((rows, columns), jnp.float32),
                       pltpu.VMEM((1, columns), jnp.float32)),
            in_specs=[pl.BlockSpec(memory_space=pltpu.HBM)] * 2,
            out_specs=(pl.BlockSpec(memory_space=pltpu.VMEM),) * 2,
            scratch_shapes=[
                pltpu.VMEM((n_ba, rows, width), jnp.bfloat16),
                pltpu.VMEM((n_ga * depth, columns), jnp.bfloat16),
                pltpu.VMEM((n_ga, 1, columns), jnp.float32),
                dma((n_ga * CHUNKS,)),
                dma((2, line)),
                dma((2, n_ga)),
                dma((lanes - 1, line)),
                dma((n_ba,)),
                dma((n_ba // 2 - 1,)),
                dma((n_ba,)),
                dma((n_ga,)),
                dma((n_ga,)),
                dma((2,)),
            ],
            compiler_params=pltpu.CompilerParams(
                collective_id=0, has_side_effects=True, vmem_limit_bytes=48 * 2**20),
        )(*(pltpu.with_memory_space_constraint(x, pltpu.HBM) for x in (coef, rot)))
        return (rotated * (1.0 / rms)).astype(jnp.bfloat16), rms.reshape(columns)

    return jax.shard_map(body, mesh=mesh, in_specs=(P("ga", "ba"), P("ga", "ba")),
                         out_specs=(P("ga", "ba"), P("ba")), check_vma=False)
```

```python
import functools
import math

import jax
import jax.numpy as jnp
from jax import lax
from jax.experimental import pallas as pl
from jax.experimental.pallas import tpu as pltpu
from jax.sharding import PartitionSpec as P

MESH = pl.DeviceIdType.MESH
CHUNKS = 6
CROSS = 1


def kernel(n_ga, n_ba, line, coef, rot, total, rms_out, a_buf, b_buf, stats,
           recv, send_z, send_zb, send_y, a_recv, a_send_x, a_send_p, s_recv, s_send, own):
    lanes = n_ga // line
    depth = rot.shape[0]
    rows, width = coef.shape
    piece = depth // CHUNKS
    span = lanes * depth
    me, mb = lax.axis_index("ga"), lax.axis_index("ba")
    z, w = me // lanes, lax.rem(me, lanes)
    bx, bc = mb // 2, lax.rem(mb, 2)
    half = n_ba // 2

    def ga(i):
        return {"ga": i}

    def side(o):
        return lax.rem(w + o, lanes)

    def chunk(index):
        return b_buf.at[pl.ds(pl.multiple_of(index * piece, piece), piece)]

    partner = mb + 1 - 2 * bc
    far = [lax.rem(bx + o, half) * 2 + bc for o in range(1, half)]

    barrier = pltpu.get_barrier_semaphore()
    def greet(device):
        pl.semaphore_signal(barrier, inc=1, device_id=device, device_id_type=MESH)

    @pl.when(z > 0)
    def _():
        greet(ga(me - lanes))

    @pl.when(z < line - 1)
    def _():
        greet(ga(me + lanes))

    for o in range(1, lanes):
        greet(ga(z * lanes + side(o)))
    for target in [*far, partner]:
        greet({"ba": target})

    mine = [
        pltpu.make_async_copy(rot, b_buf.at[pl.ds(pl.multiple_of(me * depth, depth), depth)], own.at[0]),
        pltpu.make_async_copy(coef, a_buf.at[mb], own.at[1]),
    ]
    ends = (line - 1 - z) // (line - 1) + z // (line - 1)
    pl.semaphore_wait(barrier, 2 - ends + lanes - 1 + len(far) + 1)

    def remote(src, index, sem, target):
        return pltpu.make_async_remote_copy(
            src_ref=src, dst_ref=chunk(index), send_sem=sem, recv_sem=recv.at[index],
            device_id=ga(target), device_id_type=MESH)

    def arrived(index):
        pltpu.make_async_copy(chunk(index), chunk(index), recv.at[index]).wait()

    def along(k, src, index, sem):
        @pl.when(z < line - 1 if k == 0 else z > 0)
        def _():
            remote(src, index, sem, me + lanes if k == 0 else me - lanes).start()

    def across(src, index, from_z):
        for o in range(1, lanes):
            remote(src, index, send_y.at[o - 1, from_z], z * lanes + side(o)).start()

    def own_chunk(q):
        return rot.at[pl.ds(q * piece, piece)]

    last = CHUNKS - CROSS
    crossed = [(o, q) for q in range(last, CHUNKS) for o in range(1, lanes)]
    for q in range(last, CHUNKS):
        across(own_chunk(q), me * CHUNKS + q, z)
    for q in range(CHUNKS):
        for k in range(2):
            along(k, own_chunk(q), me * CHUNKS + q, send_z.at[k, z])
        if q < last:
            across(own_chunk(q), me * CHUNKS + q, z)

    def a_copy(src, index, sem, target):
        return pltpu.make_async_remote_copy(
            src_ref=src, dst_ref=a_buf.at[index], send_sem=sem, recv_sem=a_recv.at[index],
            device_id={"ba": target}, device_id_type=MESH)

    for o, target in enumerate(far):
        a_copy(coef, mb, a_send_x.at[o], target).start()
    a_copy(coef, mb, a_send_p.at[mb], partner).start()
    for copy in mine:
        copy.start()

    for o, q in crossed:
        index = (z * lanes + side(o)) * CHUNKS + q
        arrived(index)
        for k in range(2):
            along(k, chunk(index), index, send_zb.at[k, z * lanes + side(o)])

    tile = math.gcd(rows, 1280)

    def multiply(j, dist, part):
        from_z = z - dist + 2 * dist * j

        @pl.when((from_z >= 0) & (from_z < line) & ((dist > 0) | (j == 0)))
        def _():
            if part == "all":
                for o in range(1, lanes):
                    for q in range(last):
                        arrived((from_z * lanes + side(o)) * CHUNKS + q)
                panel(from_z * span, span, dist)
                return
            if part == "own":
                panel((from_z * lanes + w) * depth, depth, dist)
                return
            for o in range(1, lanes):
                block = from_z * lanes + side(o)
                for q in range(cut) if part == "cut" else range(cut, last):
                    arrived(block * CHUNKS + q)
                if part == "cut":
                    panel(block * depth, cut * piece, dist)
                else:
                    panel(block * depth + cut * piece, depth - cut * piece, dist)

    cut = max(q for q in range(last) if q * piece % 128 == 0) if depth % 128 == 0 else 0

    def panel(begin, size, dist):
        at, column = begin // width, pl.multiple_of(lax.rem(begin, width), 128)

        @pl.loop(0, rows // tile)
        def _(t):
            part = pl.ds(pl.multiple_of(t * tile, tile), tile)
            product = jnp.dot(
                a_buf[at, part, pl.ds(column, size)],
                b_buf[pl.ds(pl.multiple_of(begin, 128), size), :],
                preferred_element_type=jnp.float32)

            @pl.when(dist == 0)
            def _():
                total[part, :] = product

            @pl.when(dist > 0)
            def _():
                total[part, :] += product

    def at_distance(dist, part="all"):
        if cut == 0:
            if part in ("own", "cut"):
                return
            part = "all"
        lax.fori_loop(0, 2, lambda j, c: (multiply(j, dist, part), c)[1], 0)

    def relay(d, carry):
        for step, (o, q) in enumerate([(0, q) for q in range(CHUNKS)] + crossed):
            for k in range(2):
                from_z = z - d if k == 0 else z + d

                @pl.when((from_z >= 0) & (from_z < line))
                def _():
                    block = from_z * lanes + side(o)
                    index = block * CHUNKS + q
                    arrived(index)
                    along(k, chunk(index), index, send_zb.at[k, block] if o else send_z.at[k, from_z])
                    if q < last:
                        across(chunk(index), index, from_z)

            if step == CHUNKS // 3:
                @pl.when(d == 2)
                def _():
                    for source in far:
                        pltpu.make_async_copy(a_buf.at[source], a_buf.at[source], a_recv.at[source]).wait()
                        a_copy(a_buf.at[source], source, a_send_p.at[source], partner).start()

            if step == CHUNKS // 6:
                @pl.when(d == line - 1)
                def _():
                    at_distance(line - 3)

            for when, dist, part in ((CHUNKS // 2, line - 2, "own"), (CHUNKS - 2, line - 2, "cut"),
                                     (CHUNKS - 2, line - 2, "rest"), (CHUNKS - 1, line - 1, "own"),
                                     (CHUNKS - 1, line - 1, "cut")):
                if step == when:
                    @pl.when(d == line - 1)
                    def _():
                        at_distance(dist, part)

            if step == CHUNKS - 1:
                @pl.when(d == 2)
                def _():
                    for copy in mine:
                        copy.wait()
                    for x in range(half):
                        source = x * 2 + 1 - bc
                        pltpu.make_async_copy(a_buf.at[source], a_buf.at[source], a_recv.at[source]).wait()

                @pl.when((d >= 2) & (d < line - 1))
                def _():
                    at_distance(d - 2)
        return carry

    lax.fori_loop(1, line, relay, 0)
    at_distance(line - 1, "rest")

    def squares(t, c):
        v = total[pl.ds(pl.multiple_of(t * tile, tile), tile), :]
        return c + jnp.sum(v * v, axis=0, keepdims=True)

    stats[me] = lax.fori_loop(0, rows // tile, squares, jnp.zeros((1, total.shape[1]), jnp.float32))

    def share(o, target, slot):
        return pltpu.make_async_remote_copy(
            src_ref=stats.at[me], dst_ref=stats.at[me], send_sem=s_send.at[o], recv_sem=s_recv.at[slot],
            device_id=ga(target), device_id_type=MESH)

    for o in range(1, n_ga):
        share(o, lax.rem(me + o, n_ga), me).start()
    for o in range(1, n_ga):
        source = lax.rem(me + o, n_ga)
        pltpu.make_async_copy(stats.at[source], stats.at[source], s_recv.at[source]).wait()
    everything = stats[0]
    for g in range(1, n_ga):
        everything = everything + stats[g]
    rms = jnp.sqrt(everything / (rows * n_ga) + 1e-06)
    rms_out[...] = rms
    for o in range(1, n_ga):
        share(o, lax.rem(me + o, n_ga), me).wait_send()
    for o, target in enumerate(far):
        a_copy(coef, mb, a_send_x.at[o], target).wait_send()
    for x in range(half):
        a_copy(coef, x * 2 + bc, a_send_p.at[x * 2 + bc], partner).wait_send()

    def sent(count, sem):
        view = b_buf.at[pl.ds(0, count * piece)]
        pltpu.make_async_copy(view, view, sem).wait()

    for from_z in range(line):
        for k in range(2):
            @pl.when((z >= from_z) & (z < line - 1) if k == 0 else (z <= from_z) & (z > 0))
            def _():
                sent(CHUNKS, send_z.at[k, from_z])
                for o in range(1, lanes):
                    sent(CROSS, send_zb.at[k, from_z * lanes + side(o)])
        for o in range(1, lanes):
            @pl.when(z == from_z)
            def _():
                sent(CHUNKS, send_y.at[o - 1, from_z])

            @pl.when(z != from_z)
            def _():
                sent(last, send_y.at[o - 1, from_z])


def solution(mesh):
    n_ga, n_ba = mesh.shape["ga"], mesh.shape["ba"]
    line = 2 ** math.ceil(math.log2(n_ga) / 2)
    lanes = n_ga // line

    def body(coef, rot):
        rows, width = coef.shape
        depth, columns = rot.shape
        dma = pltpu.SemaphoreType.DMA
        rotated, rms = pl.pallas_call(
            functools.partial(kernel, n_ga, n_ba, line),
            out_shape=(pltpu.VMEM((rows, columns), jnp.float32),
                       pltpu.VMEM((1, columns), jnp.float32)),
            in_specs=[pl.BlockSpec(memory_space=pltpu.HBM)] * 2,
            out_specs=(pl.BlockSpec(memory_space=pltpu.VMEM),) * 2,
            scratch_shapes=[
                pltpu.VMEM((n_ba, rows, width), jnp.bfloat16),
                pltpu.VMEM((n_ga * depth, columns), jnp.bfloat16),
                pltpu.VMEM((n_ga, 1, columns), jnp.float32),
                dma((n_ga * CHUNKS,)),
                dma((2, line)),
                dma((2, n_ga)),
                dma((lanes - 1, line)),
                dma((n_ba,)),
                dma((n_ba // 2 - 1,)),
                dma((n_ba,)),
                dma((n_ga,)),
                dma((n_ga,)),
                dma((2,)),
            ],
            compiler_params=pltpu.CompilerParams(
                collective_id=0, has_side_effects=True, vmem_limit_bytes=48 * 2**20),
        )(*(pltpu.with_memory_space_constraint(x, pltpu.HBM) for x in (coef, rot)))
        return (rotated * (1.0 / rms)).astype(jnp.bfloat16), rms.reshape(columns)

    return jax.shard_map(body, mesh=mesh, in_specs=(P("ga", "ba"), P("ga", "ba")),
                         out_specs=(P("ga", "ba"), P("ba")), check_vma=False)
```
